32 devices in a mesh: row: 4 (over z), col: 8 (over y, x, core).
Axes of the slice: x: 2, y: 2, z: 4, core: 2. Of those that a mesh axis runs over, the one named last changes fastest.
Arguments:
- band_sites: float32 [2, 128], P(None, 'row'), may hold values from 0 to 1
- test_sites: float32 [2, 1024], P(None, 'col'), may hold values from 0 to 1
- band_factor: float32 [128, 128], P('row', 'col'), as said below
- prior_factor: float32 [128, 2048], P('row', 'col'), may hold values from -0.125 to 0.125
- prior_solution: float32 [2048, 1024], P('col', 'row'), may hold values from -6 to 6
- prior_covariance: float32 [1024, 1024], P('row', 'col'), may hold values from -4 to 4
Outputs:
- band_solution: float32 [128, 1024], P('row', 'col')
- covariance: float32 [1024, 1024], P('row', 'col')
The draws below stay inside these ranges and needn't reach their ends.
Inputs may be any that keep to these rules, and one draw needn't show every extreme that they name: band_factor is lower triangular with diagonal entries in 1 to 2 and small entries below it.
All inputs are finite; a program needn't handle non-finite values.
Results may differ from the reference program's by a relative error of at most 0.00011.
Values sent between devices are 32-bit elements; how exact they have to be, the bound alone decides.
No kernel may reach another device: no remote copies, remote signals or barrier semaphores. Data moves between devices by JAX's collectives and lax.ppermute only.
A program may use at most 64 MiB of HBM per device.

```python
import jax
import jax.numpy as jnp
from jax import lax

BAND = 128
TESTS = 1024
PREV = 2048


def draw_band_factor(key, part):
    first_key = jax.random.fold_in(key, 11)
    second_key = jax.random.fold_in(key, 23)
    lower_part = jax.random.normal(first_key, (BAND, BAND), jnp.float32) * (0.5 / BAND ** 0.5)
    row_index = jnp.arange(BAND)[:, None]
    col_index = jnp.arange(BAND)[None, :]
    lower_part = jnp.where(row_index > col_index, lower_part, 0.0)
    diagonal = jax.random.uniform(second_key, (BAND,), jnp.float32, 1.0, 2.0)
    return lower_part + jnp.diag(diagonal)


def spiked(drawn, stream_key, source, target, parts, factor):
    def block_of(axis_at):
        return (jnp.arange(drawn.shape[axis_at]) // (drawn.shape[axis_at] // parts)).reshape((-1,) + (1,) * (drawn.ndim - 1 - axis_at))

    one_side = jax.random.permutation(stream_key, parts)[block_of(target)]
    second = (block_of(target) + parts // 2) % parts
    return jnp.where((block_of(source) == one_side) | (block_of(source) == second), factor * drawn, drawn)


def level_of(rng, shape, pieces, low, largest):
    def one(position, shards_of):
        heights = jax.random.uniform(jax.random.fold_in(jax.random.fold_in(rng, 6), position), (shards_of,), jnp.float32, low / len(pieces), largest / len(pieces))
        return jnp.repeat(jnp.exp(heights), shape[position] // shards_of).reshape((-1,) + (1,) * (len(shape) - position - 1))

    level = one(*pieces[0])
    for cut in pieces[1:]:
        level = level * one(*cut)
    return level


def normal_values(rng, extent, scale, limit, cuts=(), held_as=jnp.bfloat16):
    entries = jax.random.normal(rng, extent, jnp.float32) * scale
    if len(cuts) > 0:
        entries = level_of(rng, extent, cuts, -0.22, 0.18) * entries
    return jnp.clip(entries, min=-limit, max=limit).astype(held_as)


def bell_draw_with(own_key, dims, scale, limit, cuts, heavy, kind=jnp.bfloat16):
    drawn = scale * jax.random.normal(own_key, dims, jnp.float32)
    if cuts:
        drawn = drawn * level_of(own_key, dims, cuts, -0.22, 0.18)
    return jnp.clip(spiked(drawn, jax.random.fold_in(own_key, 3), *heavy), -limit, limit).astype(kind)


def setup_inputs(seed: int = 0) -> dict:
    streams_of = jax.random.split(jax.random.key(seed), 7)
    band_sites = jnp.clip(1.0 * jax.random.uniform(streams_of[0], (2, BAND), jnp.float32) ** level_of(streams_of[0], (2, BAND), ((1, 4),), -0.2, 0.2), 0.0, 1.0)
    test_sites = jnp.clip(1.0 * jax.random.uniform(streams_of[1], (2, TESTS), jnp.float32) ** level_of(streams_of[1], (2, TESTS), ((1, 8),), -0.2, 0.2), 0.0, 1.0)
    band_factor = draw_band_factor(jax.random.fold_in(streams_of[6], 71), 0)
    prior_factor = normal_values(streams_of[3], (BAND, PREV), PREV ** -0.5, 0.125, ((0, 4), (1, 8)), jnp.float32)
    prior_solution = bell_draw_with(streams_of[4], (PREV, TESTS), 1.0, 6.0, ((0, 8), (1, 4)), (0, 1, 8, 2.0), jnp.float32)
    prior_covariance = normal_values(streams_of[5], (TESTS, TESTS), 0.5, 4.0, ((0, 4), (1, 8)), jnp.float32)
    return dict(band_sites=band_sites, test_sites=test_sites, band_factor=band_factor, prior_factor=prior_factor, prior_solution=prior_solution, prior_covariance=prior_covariance)


length_scale = 0.3

def matern(band_sites, test_sites):
    delta_x = band_sites[0][:, None] - test_sites[0][None, :]
    delta_y = band_sites[1][:, None] - test_sites[1][None, :]
    scaled = jnp.sqrt(delta_x * delta_x + delta_y * delta_y + 1e-06) * (3.0 ** 0.5 / length_scale)
    return (1.0 + scaled) * jnp.exp(-scaled)

def reference(band_sites, test_sites, band_factor, prior_factor, prior_solution, prior_covariance):
    cross = matern(band_sites, test_sites)
    update = jnp.dot(prior_factor.astype(jnp.float32), prior_solution.astype(jnp.float32), precision=lax.Precision.HIGHEST, preferred_element_type=jnp.float32)
    remaining = cross - update
    band_solution = lax.linalg.triangular_solve(band_factor, remaining, left_side=True, lower=True)
    gram_sum = lax.dot_general(band_solution.astype(jnp.float32), band_solution.astype(jnp.float32), (((0,), (0,)), ((), ())), precision=lax.Precision.HIGHEST, preferred_element_type=jnp.float32)
    return (band_solution, prior_covariance - gram_sum)
```

```python
import jax
import jax.numpy as jnp
from jax import lax
from jax.sharding import PartitionSpec as P

length_scale = 0.3
HIGHEST = lax.Precision.HIGHEST


def matern(band_sites, test_sites):
    delta_x = band_sites[0][:, None] - test_sites[0][None, :]
    delta_y = band_sites[1][:, None] - test_sites[1][None, :]
    scaled = jnp.sqrt(delta_x * delta_x + delta_y * delta_y + 1e-06) * (3.0**0.5 / length_scale)
    return (1.0 + scaled) * jnp.exp(-scaled)


def dot(a, b, contract=((1,), (0,))):
    return lax.dot_general(a, b, (contract, ((), ())), precision=HIGHEST, preferred_element_type=jnp.float32)


def permute(x, rows, cols, target):
    pairs = []
    for r in range(rows):
        for c in range(cols):
            to_r, to_c = target(r, c)
            pairs.append((r * cols + c, to_r * cols + to_c))
    return lax.ppermute(x, ("row", "col"), pairs)


def stages(count):
    out, stride = [], 1
    while stride < count:
        radix = 4 if stride * 4 <= count else 2
        out.append((stride, radix))
        stride *= radix
    return out


def natural(blocks, index):
    count = blocks.shape[0]
    bit = 1
    while bit < count:
        split = blocks.reshape((count // (2 * bit), 2, bit) + blocks.shape[1:])
        blocks = jnp.where((index & bit) != 0, split[:, ::-1], split).reshape(blocks.shape)
        bit *= 2
    return blocks


def gather(x, rows, cols, count, step):
    blocks = x[None]
    for stride, radix in stages(count):
        blocks = jnp.concatenate([blocks] + [permute(blocks, rows, cols, step(d * stride)) for d in range(1, radix)])
    return blocks


def reduce_all(x, rows, cols, count, step):
    for stride, radix in stages(count):
        x = sum([permute(x, rows, cols, step(d * stride)) for d in range(1, radix)], x)
    return x


def lower_inverse(t):
    size = t.shape[0]
    row = lax.broadcasted_iota(jnp.int32, t.shape, 0)
    col = lax.broadcasted_iota(jnp.int32, t.shape, 1)
    inverse = jnp.where(row == col, 1.0 / t, 0.0)
    block = 1
    while block < size:
        below = (row // (2 * block) == col // (2 * block)) & (row // block > col // block)
        inverse = inverse - dot(dot(inverse, jnp.where(below, t, 0.0)), inverse)
        block *= 2
    return inverse


def local(band_sites, test_sites, band_factor, prior_factor, prior_solution, prior_covariance):
    rows, cols = lax.axis_size("row"), lax.axis_size("col")
    tile = test_sites.shape[1]
    band = band_factor.shape[0] * rows
    r, c = lax.axis_index("row"), lax.axis_index("col")
    q, k = c // 2, c % 2

    def along_row(d):
        return lambda i, j: (i ^ d, j)

    def along_col(d):
        return lambda i, j: (i, j ^ (2 * d))

    def other_core(i, j):
        return i, j ^ 1

    factor = natural(gather(prior_factor, rows, cols, rows, along_row), r).reshape(band, -1)
    t_row = natural(gather(band_factor, rows, cols, rows, along_row), r).reshape(band, -1)
    sites = natural(gather(band_sites, rows, cols, rows, along_row), r).transpose(1, 0, 2).reshape(2, band)

    halves = prior_solution.reshape(-1, 2, tile)
    mine = dot(factor, lax.dynamic_index_in_dim(halves, k, 1, keepdims=False))
    theirs = dot(factor, lax.dynamic_index_in_dim(halves, 1 - k, 1, keepdims=False))
    part = mine + permute(theirs, rows, cols, other_core)
    cross = jnp.where(q == r, matern(sites, test_sites), 0.0)
    rest = reduce_all(cross - part, rows, cols, cols // 2, along_col)

    t_pair = jnp.stack([t_row, permute(t_row, rows, cols, other_core)])
    t_pair = natural(t_pair, k).transpose(1, 0, 2).reshape(band, -1)
    t_full = natural(gather(t_pair, rows, cols, cols // 2, along_col), q).transpose(1, 0, 2).reshape(band, band)

    rest_other = permute(rest, rows, cols, other_core)
    moved = permute(rest, rows, cols, lambda i, j: ((j // 2) ^ (rows - 1), 2 * i + j % 2))
    rest_c = jnp.where(q == r, rest, moved)
    inverse = lower_inverse(t_full)
    both = natural(jnp.stack([rest, rest_other]), k)
    left = jnp.concatenate([dot(inverse, both[0]), dot(inverse, both[1])], axis=1)
    right = dot(inverse, rest_c)
    band_solution = lax.dynamic_slice_in_dim(right, r * (band // rows), band // rows, 0)
    return band_solution, prior_covariance - dot(left, right, ((0,), (0,)))


def solution(mesh):
    placed = (
        P(None, "row"),
        P(None, "col"),
        P("row", "col"),
        P("row", "col"),
        P("col", "row"),
        P("row", "col"),
    )
    return jax.shard_map(
        local,
        mesh=mesh,
        in_specs=placed,
        out_specs=(P("row", "col"), P("row", "col")),
        check_vma=False,
    )
```

```python
import jax
import jax.numpy as jnp
from jax import lax
from jax.sharding import PartitionSpec as P

length_scale = 0.3
HIGHEST = lax.Precision.HIGHEST


def matern(band_sites, test_sites):
    delta_x = band_sites[0][:, None] - test_sites[0][None, :]
    delta_y = band_sites[1][:, None] - test_sites[1][None, :]
    scaled = jnp.sqrt(delta_x * delta_x + delta_y * delta_y + 1e-06) * (3.0**0.5 / length_scale)
    return (1.0 + scaled) * jnp.exp(-scaled)


def dot(a, b, contract=((1,), (0,))):
    return lax.dot_general(a, b, (contract, ((), ())), precision=HIGHEST, preferred_element_type=jnp.float32)


def permute(x, rows, cols, target):
    pairs = []
    for r in range(rows):
        for c in range(cols):
            to_r, to_c = target(r, c)
            pairs.append((r * cols + c, to_r * cols + to_c))
    return lax.ppermute(x, ("row", "col"), pairs)


def stages(count):
    out, stride = [], 1
    while stride < count:
        radix = 4 if stride * 4 <= count else 2
        out.append((stride, radix))
        stride *= radix
    return out


def natural(blocks, index):
    count = blocks.shape[0]
    bit = 1
    while bit < count:
        split = blocks.reshape((count // (2 * bit), 2, bit) + blocks.shape[1:])
        blocks = jnp.where((index & bit) != 0, split[:, ::-1], split).reshape(blocks.shape)
        bit *= 2
    return blocks


def gather(x, rows, cols, count, step):
    blocks = x[None]
    for stride, radix in stages(count):
        blocks = jnp.concatenate([blocks] + [permute(blocks, rows, cols, step(d * stride)) for d in range(1, radix)])
    return blocks


def reduce_and_gather(x, extra, rows, cols, count, step):
    blocks, height = extra[None], x.shape[0]
    for stride, radix in stages(count):
        sent = jnp.concatenate([x, blocks.reshape(-1, x.shape[1])])
        got = [permute(sent, rows, cols, step(d * stride)) for d in range(1, radix)]
        x = sum([g[:height] for g in got], x)
        blocks = jnp.concatenate([blocks] + [g[height:].reshape(blocks.shape) for g in got])
    return x, blocks


def lower_inverse_t(u):
    size = u.shape[0]
    row = lax.broadcasted_iota(jnp.int32, u.shape, 0)
    col = lax.broadcasted_iota(jnp.int32, u.shape, 1)
    inverse = jnp.where(row == col, 1.0 / u, 0.0)
    block = 1
    while block < size:
        above = (row // (2 * block) == col // (2 * block)) & (row // block < col // block)
        inverse = inverse - dot(dot(inverse, jnp.where(above, u, 0.0)), inverse)
        block *= 2
    return inverse


def pack(prior_factor, band_factor, band_sites):
    width = prior_factor.shape[1]
    turned = band_factor.T
    parts = [turned[i : i + 8] for i in range(0, turned.shape[0], 8)]
    parts.append(jnp.pad(band_sites, ((0, 8 - band_sites.shape[0]), (0, 0))))
    low = jnp.concatenate(parts, axis=1)
    low = jnp.pad(low, ((0, 0), (0, width - low.shape[1])))
    return jnp.concatenate([prior_factor, low])


def unpack(blocks, tile_rows, tile_cols):
    factor = blocks[:, :tile_rows].reshape(-1, blocks.shape[2])
    low = blocks[:, tile_rows:].transpose(1, 0, 2)
    lanes = lambda i: low[:, :, i * tile_rows : (i + 1) * tile_rows].reshape(8, -1)
    groups = tile_cols // 8
    turned = jnp.concatenate([lanes(i) for i in range(groups)])
    return factor, turned, lanes(groups)[:2]


def local(band_sites, test_sites, band_factor, prior_factor, prior_solution, prior_covariance):
    rows, cols = lax.axis_size("row"), lax.axis_size("col")
    tile = test_sites.shape[1]
    tile_rows, tile_cols = band_factor.shape
    band = tile_rows * rows
    r, c = lax.axis_index("row"), lax.axis_index("col")
    q, k = c // 2, c % 2

    def along_row(d):
        return lambda i, j: (i ^ d, j)

    def along_col(d):
        return lambda i, j: (i, j ^ (2 * d))

    def other_core(i, j):
        return i, j ^ 1

    def to_column(i, j):
        return (j // 2) ^ (rows - 1) ^ ((i + 1) & (rows // 2)), 2 * i + j % 2

    blocks = natural(gather(pack(prior_factor, band_factor, band_sites), rows, cols, rows, along_row), r)
    factor, turned, sites = unpack(blocks, tile_rows, tile_cols)

    halves = prior_solution.reshape(-1, 2, tile)
    theirs = dot(factor, lax.dynamic_index_in_dim(halves, 1 - k, 1, keepdims=False))
    mine = dot(factor, lax.dynamic_index_in_dim(halves, k, 1, keepdims=False))
    turned = turned.reshape(-1, tile)
    got = permute(jnp.concatenate([theirs, turned]), rows, cols, other_core)
    cross = jnp.where(q == r, matern(sites, test_sites), 0.0)
    part = (cross - mine) - got[:band]
    pair = natural(jnp.stack([turned, got[band:]]), k).reshape(-1, tile)

    rest, columns = reduce_and_gather(part, pair, rows, cols, cols // 2, along_col)
    moved = permute(rest, rows, cols, to_column)
    rest_other = permute(rest, rows, cols, other_core)
    inverse = lower_inverse_t(natural(columns, q).reshape(band, band))
    first = ((0,), (0,))
    both = natural(jnp.stack([dot(inverse, rest, first), dot(inverse, rest_other, first)]), k)
    right = dot(inverse, jnp.where(q == r, rest, moved), first)
    left = jnp.concatenate([both[0], both[1]], axis=1)
    band_solution = lax.dynamic_slice_in_dim(right, r * tile_rows, tile_rows, 0)
    return band_solution, prior_covariance - dot(left, right, first)


def solution(mesh):
    placed = (
        P(None, "row"),
        P(None, "col"),
        P("row", "col"),
        P("row", "col"),
        P("col", "row"),
        P("row", "col"),
    )
    return jax.shard_map(
        local,
        mesh=mesh,
        in_specs=placed,
        out_specs=(P("row", "col"), P("row", "col")),
        check_vma=False,
    )
```

```python
import jax
import jax.numpy as jnp
from jax import lax
from jax.sharding import PartitionSpec as P

length_scale = 0.3
HIGHEST = lax.Precision.HIGHEST
HIGH = lax.Precision.HIGH
TWICE = True


def matern(band_sites, test_sites):
    delta_x = band_sites[0][:, None] - test_sites[0][None, :]
    delta_y = band_sites[1][:, None] - test_sites[1][None, :]
    scaled = jnp.sqrt(delta_x * delta_x + delta_y * delta_y + 1e-06) * (3.0**0.5 / length_scale)
    return (1.0 + scaled) * jnp.exp(-scaled)


def dot(a, b, contract=((1,), (0,)), precision=HIGHEST):
    return lax.dot_general(a, b, (contract, ((), ())), precision=precision, preferred_element_type=jnp.float32)


def permute(x, rows, cols, target):
    pairs = []
    for r in range(rows):
        for c in range(cols):
            to_r, to_c = target(r, c)
            pairs.append((r * cols + c, to_r * cols + to_c))
    return lax.ppermute(x, ("row", "col"), pairs)


def stages(count):
    out, stride = [], 1
    while stride < count:
        radix = 4 if stride * 4 <= count else 2
        out.append((stride, radix))
        stride *= radix
    return out


def natural(blocks, index):
    count = blocks.shape[0]
    bit = 1
    while bit < count:
        split = blocks.reshape((count // (2 * bit), 2, bit) + blocks.shape[1:])
        blocks = jnp.where((index & bit) != 0, split[:, ::-1], split).reshape(blocks.shape)
        bit *= 2
    return blocks


def gather(x, rows, cols, count, step):
    blocks = x[None]
    for stride, radix in stages(count):
        got = []
        for d in range(1, radix):
            got.append(permute(blocks, rows, cols, step(d * stride)))
        blocks = jnp.concatenate([blocks] + got)
    return blocks


def reduce_and_gather(x, extra, rows, cols, count, step):
    blocks, height = extra[None], x.shape[0]
    for stride, radix in stages(count):
        sent = jnp.concatenate([x, blocks.reshape(-1, x.shape[1])])
        got = []
        for d in range(1, radix):
            got.append(permute(sent, rows, cols, step(d * stride)))
        x = sum([g[:height] for g in got], x)
        blocks = jnp.concatenate([blocks] + [g[height:].reshape(blocks.shape) for g in got])
    return x, blocks


def upper_inverse(u, base=16):
    size = u.shape[0]
    row = lax.broadcasted_iota(jnp.int32, u.shape, 0)
    col = lax.broadcasted_iota(jnp.int32, u.shape, 1)
    scale = jnp.sum(jnp.where(row == col, u, 0.0), axis=0, keepdims=True)
    inside = (row // base == col // base) & (row < col)
    power = jnp.where(inside, -u / scale, 0.0)
    inverse = jnp.where(row == col, 1.0, power)
    order = 2
    while order < base:
        power = dot(power, power)
        inverse = inverse + dot(inverse, power)
        order *= 2
    down = jnp.sum(jnp.where(row == col, u, 0.0), axis=1, keepdims=True)
    inverse = inverse / down
    block = base
    while block < size:
        above = (row // (2 * block) == col // (2 * block)) & (row // block < col // block)
        inverse = inverse - dot(dot(inverse, jnp.where(above, u, 0.0)), inverse)
        block *= 2
    return inverse


def pack(prior_factor, band_factor, band_sites):
    width = prior_factor.shape[1]
    tall = band_factor.shape[0]
    sites = jnp.pad(band_sites, ((0, 8 - band_sites.shape[0]), (0, 0)))
    low = jnp.concatenate([band_factor.T, sites])
    low = low.reshape(-1, 8, tall).transpose(1, 0, 2).reshape(8, -1)
    low = jnp.pad(low, ((0, 0), (0, width - low.shape[1])))
    return jnp.concatenate([prior_factor, low])


def unpack(blocks, tile_rows, tile_cols):
    factor = blocks[:, :tile_rows].reshape(-1, blocks.shape[2])
    low = blocks[:, tile_rows:].transpose(1, 0, 2)
    lanes = lambda i: low[:, :, i * tile_rows : (i + 1) * tile_rows].reshape(8, -1)
    groups = tile_cols // 8
    turned = jnp.concatenate([lanes(i) for i in range(groups)])
    return factor, turned, lanes(groups)[:2]


def local(band_sites, test_sites, band_factor, prior_factor, prior_solution, prior_covariance):
    rows, cols = lax.axis_size("row"), lax.axis_size("col")
    tile = test_sites.shape[1]
    tile_rows, tile_cols = band_factor.shape
    band = tile_rows * rows
    r, c = lax.axis_index("row"), lax.axis_index("col")
    q, k = c // 2, c % 2

    def along_row(d):
        return lambda i, j: (i ^ d, j)

    def along_col(d):
        return lambda i, j: (i, j ^ (2 * d))

    def other_core(i, j):
        return i, j ^ 1

    def to_column(i, j):
        return (j // 2) ^ (rows - 1) ^ ((i + 1) & (rows // 2)), 2 * i + j % 2

    blocks = natural(gather(pack(prior_factor, band_factor, band_sites), rows, cols, rows, along_row), r)
    factor, turned, sites = unpack(blocks, tile_rows, tile_cols)

    halves = prior_solution.reshape(-1, 2, tile)
    theirs = dot(factor, lax.dynamic_index_in_dim(halves, 1 - k, 1, keepdims=False), precision=HIGH)
    turned = turned.reshape(-1, tile)
    got = permute(jnp.concatenate([theirs, turned]), rows, cols, other_core)
    mine = dot(factor, lax.dynamic_index_in_dim(halves, k, 1, keepdims=False), precision=HIGH)
    cross = jnp.where(q == r, matern(sites, test_sites), 0.0)
    mine = lax.optimization_barrier(cross - mine)
    part = mine - got[:band]
    pair = natural(jnp.stack([turned, got[band:]]), k).reshape(-1, tile)

    rest, columns = reduce_and_gather(part, pair, rows, cols, cols // 2, along_col)
    moved = permute(rest, rows, cols, to_column)
    rest_other = permute(rest, rows, cols, other_core)
    inverse = upper_inverse(natural(columns, q).reshape(band, band))
    first = ((0,), (0,))
    both = natural(jnp.stack([rest, rest_other]), k)
    left = jnp.concatenate([both[0], both[1]], axis=1)
    if TWICE:
        normal = dot(inverse, inverse, ((1,), (1,)))
        left = dot(normal, left, precision=HIGH)
        right = jnp.where(q == r, rest, moved)
        own = lax.dynamic_slice_in_dim(inverse, r * tile_rows, tile_rows, 1)
        band_solution = dot(own, right, first, HIGH)
    else:
        left = dot(inverse, left, first)
        right = dot(inverse, jnp.where(q == r, rest, moved), first)
        band_solution = lax.dynamic_slice_in_dim(right, r * tile_rows, tile_rows, 0)
    return band_solution, prior_covariance - dot(left, right, first, HIGH)


def solution(mesh):
    placed = (
        P(None, "row"),
        P(None, "col"),
        P("row", "col"),
        P("row", "col"),
        P("col", "row"),
        P("row", "col"),
    )
    return jax.shard_map(
        local,
        mesh=mesh,
        in_specs=placed,
        out_specs=(P("row", "col"), P("row", "col")),
        check_vma=False,
    )
```

```python
import jax
import jax.numpy as jnp
from jax import lax
from jax.experimental import pallas as pl
from jax.experimental.pallas import tpu as pltpu
from jax.sharding import PartitionSpec as P

length_scale = 0.3
HIGHEST = lax.Precision.HIGHEST
HIGH = lax.Precision.HIGH


def matern(band_sites, test_sites):
    delta_x = band_sites[0][:, None] - test_sites[0][None, :]
    delta_y = band_sites[1][:, None] - test_sites[1][None, :]
    scaled = jnp.sqrt(delta_x * delta_x + delta_y * delta_y + 1e-06) * (3.0**0.5 / length_scale)
    return (1.0 + scaled) * jnp.exp(-scaled)


def dot(a, b, contract=((1,), (0,)), precision=HIGHEST):
    return lax.dot_general(a, b, (contract, ((), ())), precision=precision, preferred_element_type=jnp.float32)


def permute(x, rows, cols, target):
    pairs = []
    for r in range(rows):
        for c in range(cols):
            to_r, to_c = target(r, c)
            pairs.append((r * cols + c, to_r * cols + to_c))
    return lax.ppermute(x, ("row", "col"), pairs)


def stages(count):
    out, stride = [], 1
    while stride < count:
        radix = 4 if stride * 4 <= count else 2
        out.append((stride, radix))
        stride *= radix
    return out


def matching(count, home, flip):
    near = sorted(range(count), key=lambda chip: (bin(chip ^ home).count("1"), -chip if flip else chip))
    far = sorted(range(count), key=lambda plane: -abs(plane - home))
    return [plane for _, plane in sorted(zip(near, far))]


def natural(blocks, index):
    count = blocks.shape[0]
    bit = 1
    while bit < count:
        split = blocks.reshape((count // (2 * bit), 2, bit) + blocks.shape[1:])
        blocks = jnp.where((index & bit) != 0, split[:, ::-1], split).reshape(blocks.shape)
        bit *= 2
    return blocks


def gather(x, rows, cols, count, step):
    blocks = x[None]
    for stride, radix in stages(count):
        got = []
        for d in range(1, radix):
            got.append(permute(blocks, rows, cols, step(d * stride)))
        blocks = jnp.concatenate([blocks] + got)
    return blocks


def reduce_and_gather(x, extra, rows, cols, count, step):
    blocks, height = extra[None], x.shape[0]
    for stride, radix in stages(count):
        sent = jnp.concatenate([x, blocks.reshape(-1, x.shape[1])])
        got = []
        for d in range(1, radix):
            got.append(permute(sent, rows, cols, step(d * stride)))
        x = sum([g[:height] for g in got], x)
        blocks = jnp.concatenate([blocks] + [g[height:].reshape(blocks.shape) for g in got])
    return x, blocks


def upper_inverse(u, base=16):
    size = u.shape[0]
    row = lax.broadcasted_iota(jnp.int32, u.shape, 0)
    col = lax.broadcasted_iota(jnp.int32, u.shape, 1)
    scale = jnp.sum(jnp.where(row == col, u, 0.0), axis=0, keepdims=True)
    inside = (row // base == col // base) & (row < col)
    power = jnp.where(inside, -u / scale, 0.0)
    inverse = jnp.where(row == col, 1.0, power)
    order = 2
    while order < base:
        power = dot(power, power)
        inverse = inverse + dot(inverse, power)
        order *= 2
    down = jnp.sum(jnp.where(row == col, u, 0.0), axis=1, keepdims=True)
    inverse = inverse / down
    block = base
    while block < size:
        above = (row // (2 * block) == col // (2 * block)) & (row // block < col // block)
        inverse = inverse - dot(dot(inverse, jnp.where(above, u, 0.0)), inverse)
        block *= 2
    return inverse


def split(x):
    high = x.astype(jnp.bfloat16)
    return high, (x - high.astype(jnp.float32)).astype(jnp.bfloat16)


def dot3(a, b):
    one = lambda x, y: jnp.dot(x, y, preferred_element_type=jnp.float32)
    return one(a[0], b[0]) + (one(a[0], b[1]) + one(a[1], b[0]))


def fetch(x):
    def body(x_ref, out_ref, sem):
        copy = pltpu.make_async_copy(x_ref, out_ref, sem)
        copy.start()
        copy.wait()

    return pl.pallas_call(
        body,
        out_shape=pltpu.VMEM(x.shape, x.dtype),
        in_specs=[pl.BlockSpec(memory_space=pl.ANY)],
        out_specs=pl.BlockSpec(memory_space=pltpu.VMEM),
        scratch_shapes=[pltpu.SemaphoreType.DMA],
        name="fetch",
    )(x)


def finish(own, left, right, prior_covariance):
    tall, tile = prior_covariance.shape
    pieces = 2
    piece = tall // pieces

    def body(own_ref, left_ref, right_ref, prior_ref, rows_ref, out_ref, rows_buf, buf, sems):
        whole = split(right_ref[...])
        rows_buf[...] = dot3(split(own_ref[...]), whole)
        copies = [pltpu.make_async_copy(rows_buf, rows_ref, sems.at[pieces])]
        copies[0].start()
        for i in range(pieces):
            part = pl.ds(i * piece, piece)
            buf[part] = prior_ref[part] - dot3(split(left_ref[part]), whole)
            copies.append(pltpu.make_async_copy(buf.at[part], out_ref.at[part], sems.at[i]))
            copies[-1].start()
        for copy in copies:
            copy.wait()

    vmem = pl.BlockSpec(memory_space=pltpu.VMEM)
    hbm = pl.BlockSpec(memory_space=pl.ANY)
    rows_shape = (own.shape[0], tile)
    return pl.pallas_call(
        body,
        out_shape=(
            jax.ShapeDtypeStruct(rows_shape, jnp.float32),
            jax.ShapeDtypeStruct(prior_covariance.shape, jnp.float32),
        ),
        in_specs=[vmem] * 4,
        out_specs=(hbm, hbm),
        scratch_shapes=[
            pltpu.VMEM(rows_shape, jnp.float32),
            pltpu.VMEM(prior_covariance.shape, jnp.float32),
            pltpu.SemaphoreType.DMA((pieces + 1,)),
        ],
        name="finish",
    )(*[pltpu.with_memory_space_constraint(x, pltpu.VMEM) for x in (own, left, right, prior_covariance)])


def pack(prior_factor, band_factor, band_sites):
    height, width = prior_factor.shape
    turned = band_factor.T
    tall, wide = turned.shape
    groups = tall // 8

    def body(factor_ref, turned_ref, sites_ref, out_ref, turned_buf, sites_buf, sems):
        copies = [
            pltpu.make_async_copy(turned_ref, turned_buf, sems.at[0]),
            pltpu.make_async_copy(sites_ref, sites_buf, sems.at[1]),
            pltpu.make_async_copy(factor_ref, out_ref.at[pl.ds(0, height)], sems.at[2]),
        ]
        for copy in copies:
            copy.start()
        out_ref[height:, :] = jnp.zeros((8, width), jnp.float32)
        copies[0].wait()
        for i in range(groups):
            out_ref[height:, i * wide : (i + 1) * wide] = turned_buf[8 * i : 8 * i + 8, :]
        copies[1].wait()
        count, span = sites_buf.shape
        out_ref[height : height + count, groups * wide : groups * wide + span] = sites_buf[...]
        copies[2].wait()

    hbm = pl.BlockSpec(memory_space=pl.ANY)
    return pl.pallas_call(
        body,
        out_shape=pltpu.VMEM((height + 8, width), jnp.float32),
        in_specs=[hbm, hbm, hbm],
        out_specs=pl.BlockSpec(memory_space=pltpu.VMEM),
        scratch_shapes=[
            pltpu.VMEM(turned.shape, jnp.float32),
            pltpu.VMEM(band_sites.shape, jnp.float32),
            pltpu.SemaphoreType.DMA((3,)),
        ],
        name="pack",
    )(prior_factor, turned, band_sites)


def unpack(blocks, tile_rows, tile_cols):
    factor = blocks[:, :tile_rows].reshape(-1, blocks.shape[2])
    low = blocks[:, tile_rows:].transpose(1, 0, 2)
    lanes = lambda i: low[:, :, i * tile_rows : (i + 1) * tile_rows].reshape(8, -1)
    groups = tile_cols // 8
    turned = jnp.concatenate([lanes(i) for i in range(groups)])
    return factor, turned, lanes(groups)[:2]


def local(band_sites, test_sites, band_factor, prior_factor, prior_solution, prior_covariance):
    rows, cols = lax.axis_size("row"), lax.axis_size("col")
    tile = test_sites.shape[1]
    tile_rows, tile_cols = band_factor.shape
    band = tile_rows * rows
    r, c = lax.axis_index("row"), lax.axis_index("col")
    q, k = c // 2, c % 2

    def along_row(d):
        return lambda i, j: (i ^ d, j)

    def along_col(d):
        return lambda i, j: (i, j ^ (2 * d))

    def other_core(i, j):
        return i, j ^ 1

    def to_column(i, j):
        return matching(rows, i, False)[j // 2], 2 * i + j % 2

    blocks = natural(gather(pack(prior_factor, band_factor, band_sites), rows, cols, rows, along_row), r)
    factor, turned, sites = unpack(blocks, tile_rows, tile_cols)

    halves = prior_solution.reshape(-1, 2, tile)
    theirs = dot(factor, lax.dynamic_index_in_dim(halves, 1 - k, 1, keepdims=False), precision=HIGH)
    turned = turned.reshape(-1, tile)
    got = permute(jnp.concatenate([theirs, turned]), rows, cols, other_core)
    mine = dot(factor, lax.dynamic_index_in_dim(halves, k, 1, keepdims=False), precision=HIGH)
    cross = jnp.where(q == r, matern(sites, test_sites), 0.0)
    mine = lax.optimization_barrier(cross - mine)
    part = mine - got[:band]
    pair = natural(jnp.stack([turned, got[band:]]), k).reshape(-1, tile)

    rest, columns = reduce_and_gather(part, pair, rows, cols, cols // 2, along_col)
    moved = permute(rest, rows, cols, to_column)
    rest_other = permute(rest, rows, cols, other_core)
    inverse = upper_inverse(natural(columns, q).reshape(band, band))
    first = ((0,), (0,))
    both = natural(jnp.stack([rest, rest_other]), k)
    left = jnp.concatenate([both[0], both[1]], axis=1)
    prior = fetch(prior_covariance)
    normal = dot(inverse, inverse, ((1,), (1,)))
    left = dot(left, normal, first, HIGH)
    own = lax.dynamic_slice_in_dim(inverse, r * tile_rows, tile_rows, 1).T
    return finish(own, left, jnp.where(q == r, rest, moved), prior)


def solution(mesh):
    placed = (
        P(None, "row"),
        P(None, "col"),
        P("row", "col"),
        P("row", "col"),
        P("col", "row"),
        P("row", "col"),
    )
    return jax.shard_map(
        local,
        mesh=mesh,
        in_specs=placed,
        out_specs=(P("row", "col"), P("row", "col")),
        check_vma=False,
    )
```

```python
import jax
import jax.numpy as jnp
from jax import lax
from jax.experimental import pallas as pl
from jax.experimental.pallas import tpu as pltpu
from jax.sharding import PartitionSpec as P

length_scale = 0.3
HIGHEST = lax.Precision.HIGHEST
HIGH = lax.Precision.HIGH


def matern(band_sites, test_sites):
    delta_x = band_sites[0][:, None] - test_sites[0][None, :]
    delta_y = band_sites[1][:, None] - test_sites[1][None, :]
    scaled = jnp.sqrt(delta_x * delta_x + delta_y * delta_y + 1e-06) * (3.0**0.5 / length_scale)
    return (1.0 + scaled) * jnp.exp(-scaled)


def dot(a, b, contract=((1,), (0,)), precision=HIGHEST):
    return lax.dot_general(a, b, (contract, ((), ())), precision=precision, preferred_element_type=jnp.float32)


def permute(x, rows, cols, target):
    pairs = []
    for r in range(rows):
        for c in range(cols):
            to_r, to_c = target(r, c)
            pairs.append((r * cols + c, to_r * cols + to_c))
    return lax.ppermute(x, ("row", "col"), pairs)


def stages(count):
    out, stride = [], 1
    while stride < count:
        radix = 4 if stride * 4 <= count else 2
        out.append((stride, radix))
        stride *= radix
    return out


def matching(count, home, flip):
    near = sorted(range(count), key=lambda chip: (bin(chip ^ home).count("1"), -chip if flip else chip))
    far = sorted(range(count), key=lambda plane: -abs(plane - home))
    return [plane for _, plane in sorted(zip(near, far))]


def natural(blocks, index):
    count = blocks.shape[0]
    bit = 1
    while bit < count:
        split = blocks.reshape((count // (2 * bit), 2, bit) + blocks.shape[1:])
        blocks = jnp.where((index & bit) != 0, split[:, ::-1], split).reshape(blocks.shape)
        bit *= 2
    return blocks


def gather(x, rows, cols, count, step):
    blocks = x[None]
    for stride, radix in stages(count):
        got = []
        for d in range(1, radix):
            got.append(permute(blocks, rows, cols, step(d * stride)))
        blocks = jnp.concatenate([blocks] + got)
    return blocks


def reduce_and_gather(x, extra, rows, cols, count, step):
    blocks, height = extra[None], x.shape[0]
    for stride, radix in stages(count):
        sent = jnp.concatenate([x, blocks.reshape(-1, x.shape[1])])
        got = []
        for d in range(1, radix):
            got.append(permute(sent, rows, cols, step(d * stride)))
        x = sum([g[:height] for g in got], x)
        blocks = jnp.concatenate([blocks] + [g[height:].reshape(blocks.shape) for g in got])
    return x, blocks


def upper_inverse(u, product, base=16):
    size = u.shape[0]
    row = lax.broadcasted_iota(jnp.int32, u.shape, 0)
    col = lax.broadcasted_iota(jnp.int32, u.shape, 1)
    scale = jnp.sum(jnp.where(row == col, u, 0.0), axis=0, keepdims=True)
    inside = (row // base == col // base) & (row < col)
    power = jnp.where(inside, -u / scale, 0.0)
    inverse = jnp.where(row == col, 1.0, power)
    order = 2
    while order < base:
        power = product(power, power)
        inverse = inverse + product(inverse, power)
        order *= 2
    down = jnp.sum(jnp.where(row == col, u, 0.0), axis=1, keepdims=True)
    inverse = inverse / down
    block = base
    while block < size:
        above = (row // (2 * block) == col // (2 * block)) & (row // block < col // block)
        inverse = inverse - product(product(inverse, jnp.where(above, u, 0.0)), inverse)
        block *= 2
    return inverse


def split(x):
    high = x.astype(jnp.bfloat16)
    return high, (x - high.astype(jnp.float32)).astype(jnp.bfloat16)


def dot3(a, b):
    one = lambda x, y: jnp.dot(x, y, preferred_element_type=jnp.float32)
    return one(a[0], b[0]) + (one(a[0], b[1]) + one(a[1], b[0]))


def invert(u, tile_rows):
    size = u.shape[0]

    def body(u_ref, own_ref, normal_ref, turned_buf):
        inverse = upper_inverse(u_ref[...], product3)
        turned = inverse.T
        turned_buf[...] = turned
        start = pl.multiple_of(lax.axis_index("row") * tile_rows, 8)
        own_ref[...] = turned_buf[pl.ds(start, tile_rows)]
        normal_ref[...] = product3(inverse, turned)

    vmem = pl.BlockSpec(memory_space=pltpu.VMEM)
    return pl.pallas_call(
        body,
        out_shape=(pltpu.VMEM((tile_rows, size), jnp.float32), pltpu.VMEM(u.shape, jnp.float32)),
        in_specs=[vmem],
        out_specs=(vmem, vmem),
        scratch_shapes=[pltpu.VMEM(u.shape, jnp.float32)],
        name="invert",
    )(pltpu.with_memory_space_constraint(u, pltpu.VMEM))


def product3(a, b):
    return dot3(split(a), split(b))


def fetch(x):
    def body(x_ref, out_ref, sem):
        copy = pltpu.make_async_copy(x_ref, out_ref, sem)
        copy.start()
        copy.wait()

    return pl.pallas_call(
        body,
        out_shape=pltpu.VMEM(x.shape, x.dtype),
        in_specs=[pl.BlockSpec(memory_space=pl.ANY)],
        out_specs=pl.BlockSpec(memory_space=pltpu.VMEM),
        scratch_shapes=[pltpu.SemaphoreType.DMA],
        name="fetch",
    )(x)


def fetch_halves(x, tile):
    shape = (x.shape[0], tile)

    def body(x_ref, mine_ref, theirs_ref, sems):
        k = lax.axis_index("col") % 2
        columns = lambda half: x_ref.at[:, pl.ds(pl.multiple_of(half * tile, 128), tile)]
        copies = [
            pltpu.make_async_copy(columns(1 - k), theirs_ref, sems.at[0]),
            pltpu.make_async_copy(columns(k), mine_ref, sems.at[1]),
        ]
        for copy in copies:
            copy.start()
        for copy in copies:
            copy.wait()

    vmem = pl.BlockSpec(memory_space=pltpu.VMEM)
    return pl.pallas_call(
        body,
        out_shape=(pltpu.VMEM(shape, x.dtype), pltpu.VMEM(shape, x.dtype)),
        in_specs=[pl.BlockSpec(memory_space=pl.ANY)],
        out_specs=(vmem, vmem),
        scratch_shapes=[pltpu.SemaphoreType.DMA((2,))],
        name="fetch_halves",
    )(x)


def first_product(blocks, theirs, tile_rows, tile_cols):
    count, _, width = blocks.shape
    band, tile = count * tile_rows, theirs.shape[1]
    groups = tile_cols // 8

    def body(blocks_ref, theirs_ref, factor_ref, product_ref, turned_ref, sites_ref):
        r = lax.axis_index("row")
        for j in range(count):
            start = pl.multiple_of((r ^ j) * tile_rows, 8)
            factor_ref[pl.ds(start, tile_rows)] = blocks_ref[j, :tile_rows]
        product_ref[...] = product3(factor_ref[...], theirs_ref[...])
        for g in range(groups + 1):
            pieces = [blocks_ref[j, tile_rows:, g * tile_rows : (g + 1) * tile_rows] for j in range(count)]
            bit = 1
            while bit < count:
                pieces = [jnp.where((r & bit) != 0, pieces[j ^ bit], pieces[j]) for j in range(count)]
                bit *= 2
            row = jnp.concatenate(pieces, axis=1)
            if g < groups:
                turned_ref[8 * g : 8 * g + 8] = row
            else:
                sites_ref[...] = row

    vmem = pl.BlockSpec(memory_space=pltpu.VMEM)
    here = lambda *shape: pltpu.VMEM(shape, jnp.float32)
    return pl.pallas_call(
        body,
        out_shape=(here(band, width), here(band, tile), here(tile_cols, band), here(8, band)),
        in_specs=[vmem, vmem],
        out_specs=(vmem,) * 4,
        name="first_product",
    )(*[pltpu.with_memory_space_constraint(x, pltpu.VMEM) for x in (blocks, theirs)])


def finish(own, left, right, prior_covariance):
    tall, tile = prior_covariance.shape
    pieces = 2
    piece = tall // pieces

    def body(own_ref, left_ref, right_ref, prior_ref, rows_ref, out_ref, rows_buf, buf, sems):
        whole = split(right_ref[...])
        rows_buf[...] = dot3(split(own_ref[...]), whole)
        copies = [pltpu.make_async_copy(rows_buf, rows_ref, sems.at[pieces])]
        copies[0].start()
        for i in range(pieces):
            part = pl.ds(i * piece, piece)
            buf[part] = prior_ref[part] - dot3(split(left_ref[part]), whole)
            copies.append(pltpu.make_async_copy(buf.at[part], out_ref.at[part], sems.at[i]))
            copies[-1].start()
        for copy in copies:
            copy.wait()

    vmem = pl.BlockSpec(memory_space=pltpu.VMEM)
    hbm = pl.BlockSpec(memory_space=pl.ANY)
    rows_shape = (own.shape[0], tile)
    return pl.pallas_call(
        body,
        out_shape=(
            jax.ShapeDtypeStruct(rows_shape, jnp.float32),
            jax.ShapeDtypeStruct(prior_covariance.shape, jnp.float32),
        ),
        in_specs=[vmem] * 4,
        out_specs=(hbm, hbm),
        scratch_shapes=[
            pltpu.VMEM(rows_shape, jnp.float32),
            pltpu.VMEM(prior_covariance.shape, jnp.float32),
            pltpu.SemaphoreType.DMA((pieces + 1,)),
        ],
        name="finish",
    )(*[pltpu.with_memory_space_constraint(x, pltpu.VMEM) for x in (own, left, right, prior_covariance)])


def pack(prior_factor, band_factor, band_sites):
    height, width = prior_factor.shape
    turned = band_factor.T
    tall, wide = turned.shape
    groups = tall // 8

    def body(factor_ref, turned_ref, sites_ref, out_ref, turned_buf, sites_buf, sems):
        copies = [
            pltpu.make_async_copy(turned_ref, turned_buf, sems.at[0]),
            pltpu.make_async_copy(sites_ref, sites_buf, sems.at[1]),
            pltpu.make_async_copy(factor_ref, out_ref.at[pl.ds(0, height)], sems.at[2]),
        ]
        for copy in copies:
            copy.start()
        out_ref[height:, :] = jnp.zeros((8, width), jnp.float32)
        copies[0].wait()
        for i in range(groups):
            out_ref[height:, i * wide : (i + 1) * wide] = turned_buf[8 * i : 8 * i + 8, :]
        copies[1].wait()
        count, span = sites_buf.shape
        out_ref[height : height + count, groups * wide : groups * wide + span] = sites_buf[...]
        copies[2].wait()

    hbm = pl.BlockSpec(memory_space=pl.ANY)
    return pl.pallas_call(
        body,
        out_shape=pltpu.VMEM((height + 8, width), jnp.float32),
        in_specs=[hbm, hbm, hbm],
        out_specs=pl.BlockSpec(memory_space=pltpu.VMEM),
        scratch_shapes=[
            pltpu.VMEM(turned.shape, jnp.float32),
            pltpu.VMEM(band_sites.shape, jnp.float32),
            pltpu.SemaphoreType.DMA((3,)),
        ],
        name="pack",
    )(prior_factor, turned, band_sites)


def local(band_sites, test_sites, band_factor, prior_factor, prior_solution, prior_covariance):
    rows, cols = lax.axis_size("row"), lax.axis_size("col")
    tile = test_sites.shape[1]
    tile_rows, tile_cols = band_factor.shape
    band = tile_rows * rows
    r, c = lax.axis_index("row"), lax.axis_index("col")
    q, k = c // 2, c % 2

    def along_row(d):
        return lambda i, j: (i ^ d, j)

    def along_col(d):
        return lambda i, j: (i, j ^ (2 * d))

    def other_core(i, j):
        return i, j ^ 1

    def to_column(i, j):
        return matching(rows, i, False)[j // 2], 2 * i + j % 2

    half, other_half = fetch_halves(prior_solution, tile)
    blocks = gather(pack(prior_factor, band_factor, band_sites), rows, cols, rows, along_row)
    factor, theirs, turned, sites = first_product(blocks, other_half, tile_rows, tile_cols)
    turned = turned.reshape(-1, tile)
    got = permute(jnp.concatenate([theirs, turned]), rows, cols, other_core)
    mine = dot(factor, half, precision=HIGH)
    cross = jnp.where(q == r, matern(sites, test_sites), 0.0)
    mine = lax.optimization_barrier(cross - mine)
    part = mine - got[:band]
    pair = natural(jnp.stack([turned, got[band:]]), k).reshape(-1, tile)

    rest, columns = reduce_and_gather(part, pair, rows, cols, cols // 2, along_col)
    moved = permute(rest, rows, cols, to_column)
    rest_other = permute(rest, rows, cols, other_core)
    triangle = natural(columns, q).reshape(band, band)
    if band <= 256:
        own, normal = invert(triangle, tile_rows)
    else:
        inverse = upper_inverse(triangle, dot)
        normal = dot(inverse, inverse, ((1,), (1,)))
        own = lax.dynamic_slice_in_dim(inverse, r * tile_rows, tile_rows, 1).T
    first = ((0,), (0,))
    both = natural(jnp.stack([rest, rest_other]), k)
    left = jnp.concatenate([both[0], both[1]], axis=1)
    prior = fetch(prior_covariance)
    left = dot(left, normal, first, HIGH)
    return finish(own, left, jnp.where(q == r, rest, moved), prior)


def solution(mesh):
    placed = (
        P(None, "row"),
        P(None, "col"),
        P("row", "col"),
        P("row", "col"),
        P("col", "row"),
        P("row", "col"),
    )
    return jax.shard_map(
        local,
        mesh=mesh,
        in_specs=placed,
        out_specs=(P("row", "col"), P("row", "col")),
        check_vma=False,
    )
```

```python
import jax
import jax.numpy as jnp
from jax import lax
from jax.experimental import pallas as pl
from jax.experimental.pallas import tpu as pltpu
from jax.sharding import PartitionSpec as P

length_scale = 0.3
HIGHEST = lax.Precision.HIGHEST
HIGH = lax.Precision.HIGH


def matern(band_sites, test_sites):
    delta_x = band_sites[0][:, None] - test_sites[0][None, :]
    delta_y = band_sites[1][:, None] - test_sites[1][None, :]
    scaled = jnp.sqrt(delta_x * delta_x + delta_y * delta_y + 1e-06) * (3.0**0.5 / length_scale)
    return (1.0 + scaled) * jnp.exp(-scaled)


def dot(a, b, contract=((1,), (0,)), precision=HIGHEST):
    return lax.dot_general(a, b, (contract, ((), ())), precision=precision, preferred_element_type=jnp.float32)


def permute(x, rows, cols, target):
    pairs = []
    for r in range(rows):
        for c in range(cols):
            to_r, to_c = target(r, c)
            pairs.append((r * cols + c, to_r * cols + to_c))
    return lax.ppermute(x, ("row", "col"), pairs)


def stages(count):
    out, stride = [], 1
    while stride < count:
        radix = 4 if stride * 4 <= count else 2
        out.append((stride, radix))
        stride *= radix
    return out


def matching(count, home, flip):
    near = sorted(range(count), key=lambda chip: (bin(chip ^ home).count("1"), -chip if flip else chip))
    far = sorted(set(range(count)) - {home}, key=lambda plane: -abs(plane - home))
    far.insert(1, home)
    return [plane for _, plane in sorted(zip(near, far))]


def natural(blocks, index):
    count = blocks.shape[0]
    bit = 1
    while bit < count:
        split = blocks.reshape((count // (2 * bit), 2, bit) + blocks.shape[1:])
        blocks = jnp.where((index & bit) != 0, split[:, ::-1], split).reshape(blocks.shape)
        bit *= 2
    return blocks


def gather(x, rows, cols, count, step):
    blocks = x[None]
    for stride, radix in stages(count):
        got = []
        for d in range(1, radix):
            got.append(permute(blocks, rows, cols, step(d * stride)))
        blocks = jnp.concatenate([blocks] + got)
    return blocks


def reduce_and_gather(x, extra, rows, cols, count, step):
    blocks, height = extra[None], x.shape[0]
    for stride, radix in stages(count):
        sent = jnp.concatenate([x, blocks.reshape(-1, x.shape[1])])
        got = []
        for d in range(1, radix):
            got.append(permute(sent, rows, cols, step(d * stride)))
        x = sum([g[:height] for g in got], x)
        blocks = jnp.concatenate([blocks] + [g[height:].reshape(blocks.shape) for g in got])
    return x, blocks


def upper_inverse(u, product, base=16):
    size = u.shape[0]
    row = lax.broadcasted_iota(jnp.int32, u.shape, 0)
    col = lax.broadcasted_iota(jnp.int32, u.shape, 1)
    scale = jnp.sum(jnp.where(row == col, u, 0.0), axis=0, keepdims=True)
    inside = (row // base == col // base) & (row < col)
    power = jnp.where(inside, -u / scale, 0.0)
    inverse = jnp.where(row == col, 1.0, power)
    order = 2
    while order < base:
        power = product(power, power)
        inverse = inverse + product(inverse, power)
        order *= 2
    down = jnp.sum(jnp.where(row == col, u, 0.0), axis=1, keepdims=True)
    inverse = inverse / down
    block = base
    while block < size:
        above = (row // (2 * block) == col // (2 * block)) & (row // block < col // block)
        inverse = inverse - product(product(inverse, jnp.where(above, u, 0.0)), inverse)
        block *= 2
    return inverse


def split(x):
    high = x.astype(jnp.bfloat16)
    return high, (x - high.astype(jnp.float32)).astype(jnp.bfloat16)


def dot3(a, b):
    one = lambda x, y: jnp.dot(x, y, preferred_element_type=jnp.float32)
    return one(a[0], b[0]) + (one(a[0], b[1]) + one(a[1], b[0]))


def invert(u, tile_rows):
    size = u.shape[0]

    def body(u_ref, own_ref, normal_ref, turned_buf):
        inverse = upper_inverse(u_ref[...], product3)
        turned = inverse.T
        turned_buf[...] = turned
        start = pl.multiple_of(lax.axis_index("row") * tile_rows, 8)
        own_ref[...] = turned_buf[pl.ds(start, tile_rows)]
        normal_ref[...] = product3(inverse, turned)

    vmem = pl.BlockSpec(memory_space=pltpu.VMEM)
    return pl.pallas_call(
        body,
        out_shape=(pltpu.VMEM((tile_rows, size), jnp.float32), pltpu.VMEM(u.shape, jnp.float32)),
        in_specs=[vmem],
        out_specs=(vmem, vmem),
        scratch_shapes=[pltpu.VMEM(u.shape, jnp.float32)],
        name="invert",
    )(pltpu.with_memory_space_constraint(u, pltpu.VMEM))


def product3(a, b):
    return dot3(split(a), split(b))


def fetch(x):
    def body(x_ref, out_ref, sem):
        copy = pltpu.make_async_copy(x_ref, out_ref, sem)
        copy.start()
        copy.wait()

    return pl.pallas_call(
        body,
        out_shape=pltpu.VMEM(x.shape, x.dtype),
        in_specs=[pl.BlockSpec(memory_space=pl.ANY)],
        out_specs=pl.BlockSpec(memory_space=pltpu.VMEM),
        scratch_shapes=[pltpu.SemaphoreType.DMA],
        name="fetch",
    )(x)


def fetch_halves(x, tile):
    shape = (x.shape[0], tile)

    def body(x_ref, mine_ref, theirs_ref, sems):
        k = lax.axis_index("col") % 2
        columns = lambda half: x_ref.at[:, pl.ds(pl.multiple_of(half * tile, 128), tile)]
        copies = [
            pltpu.make_async_copy(columns(1 - k), theirs_ref, sems.at[0]),
            pltpu.make_async_copy(columns(k), mine_ref, sems.at[1]),
        ]
        for copy in copies:
            copy.start()
        for copy in copies:
            copy.wait()

    vmem = pl.BlockSpec(memory_space=pltpu.VMEM)
    return pl.pallas_call(
        body,
        out_shape=(pltpu.VMEM(shape, x.dtype), pltpu.VMEM(shape, x.dtype)),
        in_specs=[pl.BlockSpec(memory_space=pl.ANY)],
        out_specs=(vmem, vmem),
        scratch_shapes=[pltpu.SemaphoreType.DMA((2,))],
        name="fetch_halves",
    )(x)


def first_product(blocks, theirs, tile_rows, tile_cols):
    count, _, width = blocks.shape
    band, tile = count * tile_rows, theirs.shape[1]
    groups = tile_cols // 8

    def body(blocks_ref, theirs_ref, factor_ref, product_ref, turned_ref, sites_ref):
        r = lax.axis_index("row")
        for j in range(count):
            start = pl.multiple_of((r ^ j) * tile_rows, 8)
            factor_ref[pl.ds(start, tile_rows)] = blocks_ref[j, :tile_rows]
        product_ref[...] = product3(factor_ref[...], theirs_ref[...])
        for g in range(groups + 1):
            pieces = [blocks_ref[j, tile_rows:, g * tile_rows : (g + 1) * tile_rows] for j in range(count)]
            bit = 1
            while bit < count:
                pieces = [jnp.where((r & bit) != 0, pieces[j ^ bit], pieces[j]) for j in range(count)]
                bit *= 2
            row = jnp.concatenate(pieces, axis=1)
            if g < groups:
                turned_ref[8 * g : 8 * g + 8] = row
            else:
                sites_ref[...] = row

    vmem = pl.BlockSpec(memory_space=pltpu.VMEM)
    here = lambda *shape: pltpu.VMEM(shape, jnp.float32)
    return pl.pallas_call(
        body,
        out_shape=(here(band, width), here(band, tile), here(tile_cols, band), here(8, band)),
        in_specs=[vmem, vmem],
        out_specs=(vmem,) * 4,
        name="first_product",
    )(*[pltpu.with_memory_space_constraint(x, pltpu.VMEM) for x in (blocks, theirs)])


def finish(own, left, right, prior_covariance):
    tall, tile = prior_covariance.shape
    pieces = 2
    piece = tall // pieces

    def body(own_ref, left_ref, right_ref, prior_ref, rows_ref, out_ref, rows_buf, buf, sems):
        whole = split(right_ref[...])
        rows_buf[...] = dot3(split(own_ref[...]), whole)
        copies = [pltpu.make_async_copy(rows_buf, rows_ref, sems.at[pieces])]
        copies[0].start()
        for i in range(pieces):
            part = pl.ds(i * piece, piece)
            buf[part] = prior_ref[part] - dot3(split(left_ref[part]), whole)
            copies.append(pltpu.make_async_copy(buf.at[part], out_ref.at[part], sems.at[i]))
            copies[-1].start()
        for copy in copies:
            copy.wait()

    vmem = pl.BlockSpec(memory_space=pltpu.VMEM)
    hbm = pl.BlockSpec(memory_space=pl.ANY)
    rows_shape = (own.shape[0], tile)
    return pl.pallas_call(
        body,
        out_shape=(
            jax.ShapeDtypeStruct(rows_shape, jnp.float32),
            jax.ShapeDtypeStruct(prior_covariance.shape, jnp.float32),
        ),
        in_specs=[vmem] * 4,
        out_specs=(hbm, hbm),
        scratch_shapes=[
            pltpu.VMEM(rows_shape, jnp.float32),
            pltpu.VMEM(prior_covariance.shape, jnp.float32),
            pltpu.SemaphoreType.DMA((pieces + 1,)),
        ],
        name="finish",
    )(*[pltpu.with_memory_space_constraint(x, pltpu.VMEM) for x in (own, left, right, prior_covariance)])


def pack(prior_factor, band_factor, band_sites):
    height, width = prior_factor.shape
    turned = band_factor.T
    tall, wide = turned.shape
    groups = tall // 8

    def body(factor_ref, turned_ref, sites_ref, out_ref, turned_buf, sites_buf, sems):
        copies = [
            pltpu.make_async_copy(turned_ref, turned_buf, sems.at[0]),
            pltpu.make_async_copy(sites_ref, sites_buf, sems.at[1]),
            pltpu.make_async_copy(factor_ref, out_ref.at[pl.ds(0, height)], sems.at[2]),
        ]
        for copy in copies:
            copy.start()
        out_ref[height:, :] = jnp.zeros((8, width), jnp.float32)
        copies[0].wait()
        for i in range(groups):
            out_ref[height:, i * wide : (i + 1) * wide] = turned_buf[8 * i : 8 * i + 8, :]
        copies[1].wait()
        count, span = sites_buf.shape
        out_ref[height : height + count, groups * wide : groups * wide + span] = sites_buf[...]
        copies[2].wait()

    hbm = pl.BlockSpec(memory_space=pl.ANY)
    return pl.pallas_call(
        body,
        out_shape=pltpu.VMEM((height + 8, width), jnp.float32),
        in_specs=[hbm, hbm, hbm],
        out_specs=pl.BlockSpec(memory_space=pltpu.VMEM),
        scratch_shapes=[
            pltpu.VMEM(turned.shape, jnp.float32),
            pltpu.VMEM(band_sites.shape, jnp.float32),
            pltpu.SemaphoreType.DMA((3,)),
        ],
        name="pack",
    )(prior_factor, turned, band_sites)


def local(band_sites, test_sites, band_factor, prior_factor, prior_solution, prior_covariance):
    rows, cols = lax.axis_size("row"), lax.axis_size("col")
    tile = test_sites.shape[1]
    tile_rows, tile_cols = band_factor.shape
    band = tile_rows * rows
    r, c = lax.axis_index("row"), lax.axis_index("col")
    q, k = c // 2, c % 2

    def along_row(d):
        return lambda i, j: (i ^ d, j)

    def along_col(d):
        return lambda i, j: (i, j ^ (2 * d))

    def other_core(i, j):
        return i, j ^ 1

    def to_column(i, j):
        return matching(rows, i, j % 2 == 0)[j // 2], 2 * i + j % 2

    half, other_half = fetch_halves(prior_solution, tile)
    blocks = gather(pack(prior_factor, band_factor, band_sites), rows, cols, rows, along_row)
    factor, theirs, turned, sites = first_product(blocks, other_half, tile_rows, tile_cols)
    turned = turned.reshape(-1, tile)
    got = permute(jnp.concatenate([theirs, turned]), rows, cols, other_core)
    mine = dot(factor, half, precision=HIGH)
    cross = jnp.where(q == r, matern(sites, test_sites), 0.0)
    mine = lax.optimization_barrier(cross - mine)
    part = mine - got[:band]
    pair = natural(jnp.stack([turned, got[band:]]), k).reshape(-1, tile)

    rest, columns = reduce_and_gather(part, pair, rows, cols, cols // 2, along_col)
    moved = permute(rest, rows, cols, to_column)
    rest_other = permute(rest, rows, cols, other_core)
    triangle = natural(columns, q).reshape(band, band)
    if band <= 256:
        own, normal = invert(triangle, tile_rows)
    else:
        inverse = upper_inverse(triangle, dot)
        normal = dot(inverse, inverse, ((1,), (1,)))
        own = lax.dynamic_slice_in_dim(inverse, r * tile_rows, tile_rows, 1).T
    first = ((0,), (0,))
    both = natural(jnp.stack([rest, rest_other]), k)
    left = jnp.concatenate([both[0], both[1]], axis=1)
    prior = fetch(prior_covariance)
    left = dot(left, normal, first, HIGH)
    return finish(own, left, jnp.where(q == r, rest, moved), prior)


def solution(mesh):
    placed = (
        P(None, "row"),
        P(None, "col"),
        P("row", "col"),
        P("row", "col"),
        P("col", "row"),
        P("row", "col"),
    )
    return jax.shard_map(
        local,
        mesh=mesh,
        in_specs=placed,
        out_specs=(P("row", "col"), P("row", "col")),
        check_vma=False,
    )
```

```python
import jax
import jax.numpy as jnp
from jax import lax
from jax.experimental import pallas as pl
from jax.experimental.pallas import tpu as pltpu
from jax.sharding import PartitionSpec as P

length_scale = 0.3
HIGHEST = lax.Precision.HIGHEST
HIGH = lax.Precision.HIGH


def matern(band_sites, test_sites):
    delta_x = band_sites[0][:, None] - test_sites[0][None, :]
    delta_y = band_sites[1][:, None] - test_sites[1][None, :]
    scaled = jnp.sqrt(delta_x * delta_x + delta_y * delta_y + 1e-06) * (3.0**0.5 / length_scale)
    return (1.0 + scaled) * jnp.exp(-scaled)


def dot(a, b, contract=((1,), (0,)), precision=HIGHEST):
    return lax.dot_general(a, b, (contract, ((), ())), precision=precision, preferred_element_type=jnp.float32)


def permute(x, rows, cols, target):
    pairs = []
    for r in range(rows):
        for c in range(cols):
            to_r, to_c = target(r, c)
            pairs.append((r * cols + c, to_r * cols + to_c))
    return lax.ppermute(x, ("row", "col"), pairs)


def stages(count):
    out, stride = [], 1
    while stride < count:
        radix = 4 if stride * 4 <= count else 2
        out.append((stride, radix))
        stride *= radix
    return out


def matching(count, home, flip):
    near = sorted(range(count), key=lambda chip: (bin(chip ^ home).count("1"), -chip if flip else chip))
    far = sorted(set(range(count)) - {home}, key=lambda plane: -abs(plane - home))
    far.insert(1, home)
    return [plane for _, plane in sorted(zip(near, far))]


def natural(blocks, index):
    count = blocks.shape[0]
    bit = 1
    while bit < count:
        split = blocks.reshape((count // (2 * bit), 2, bit) + blocks.shape[1:])
        blocks = jnp.where((index & bit) != 0, split[:, ::-1], split).reshape(blocks.shape)
        bit *= 2
    return blocks


def gather(x, rows, cols, count, step):
    blocks = x[None]
    for stride, radix in stages(count):
        got = []
        for d in range(1, radix):
            got.append(permute(blocks, rows, cols, step(d * stride)))
        blocks = jnp.concatenate([blocks] + got)
    return blocks


def reduce_and_gather(x, extra, rows, cols, count, step):
    blocks, height = extra[None], x.shape[0]
    for stride, radix in stages(count):
        sent = jnp.concatenate([x, blocks.reshape(-1, x.shape[1])])
        got = []
        for d in range(1, radix):
            got.append(permute(sent, rows, cols, step(d * stride)))
        x = sum([g[:height] for g in got], x)
        blocks = jnp.concatenate([blocks] + [g[height:].reshape(blocks.shape) for g in got])
    return x, blocks


def upper_inverse(u, product, base=16):
    size = u.shape[0]
    row = lax.broadcasted_iota(jnp.int32, u.shape, 0)
    col = lax.broadcasted_iota(jnp.int32, u.shape, 1)
    scale = jnp.sum(jnp.where(row == col, u, 0.0), axis=0, keepdims=True)
    inside = (row // base == col // base) & (row < col)
    power = jnp.where(inside, -u / scale, 0.0)
    inverse = jnp.where(row == col, 1.0, power)
    order = 2
    while order < base:
        power = product(power, power)
        inverse = inverse + product(inverse, power)
        order *= 2
    down = jnp.sum(jnp.where(row == col, u, 0.0), axis=1, keepdims=True)
    inverse = inverse / down
    block = base
    while block < size:
        above = (row // (2 * block) == col // (2 * block)) & (row // block < col // block)
        inverse = inverse - product(product(inverse, jnp.where(above, u, 0.0)), inverse)
        block *= 2
    return inverse


def split(x):
    high = x.astype(jnp.bfloat16)
    return high, (x - high.astype(jnp.float32)).astype(jnp.bfloat16)


def dot3(a, b):
    one = lambda x, y: jnp.dot(x, y, preferred_element_type=jnp.float32)
    return one(a[0], b[0]) + (one(a[0], b[1]) + one(a[1], b[0]))


def invert(u, tile_rows):
    size = u.shape[0]

    def body(u_ref, own_ref, normal_ref, turned_buf):
        inverse = upper_inverse(u_ref[...], product3)
        turned = inverse.T
        turned_buf[...] = turned
        start = pl.multiple_of(lax.axis_index("row") * tile_rows, 8)
        own_ref[...] = turned_buf[pl.ds(start, tile_rows)]
        normal_ref[...] = product3(inverse, turned)

    vmem = pl.BlockSpec(memory_space=pltpu.VMEM)
    return pl.pallas_call(
        body,
        out_shape=(pltpu.VMEM((tile_rows, size), jnp.float32), pltpu.VMEM(u.shape, jnp.float32)),
        in_specs=[vmem],
        out_specs=(vmem, vmem),
        scratch_shapes=[pltpu.VMEM(u.shape, jnp.float32)],
        name="invert",
    )(pltpu.with_memory_space_constraint(u, pltpu.VMEM))


def product3(a, b):
    return dot3(split(a), split(b))


def fetch(x):
    def body(x_ref, out_ref, sem):
        copy = pltpu.make_async_copy(x_ref, out_ref, sem)
        copy.start()
        copy.wait()

    return pl.pallas_call(
        body,
        out_shape=pltpu.VMEM(x.shape, x.dtype),
        in_specs=[pl.BlockSpec(memory_space=pl.ANY)],
        out_specs=pl.BlockSpec(memory_space=pltpu.VMEM),
        scratch_shapes=[pltpu.SemaphoreType.DMA],
        name="fetch",
    )(x)


def fetch_halves(x, tile):
    shape = (x.shape[0], tile)

    def body(x_ref, mine_ref, theirs_ref, sems):
        k = lax.axis_index("col") % 2
        columns = lambda half: x_ref.at[:, pl.ds(pl.multiple_of(half * tile, 128), tile)]
        copies = [
            pltpu.make_async_copy(columns(1 - k), theirs_ref, sems.at[0]),
            pltpu.make_async_copy(columns(k), mine_ref, sems.at[1]),
        ]
        for copy in copies:
            copy.start()
        for copy in copies:
            copy.wait()

    vmem = pl.BlockSpec(memory_space=pltpu.VMEM)
    return pl.pallas_call(
        body,
        out_shape=(pltpu.VMEM(shape, x.dtype), pltpu.VMEM(shape, x.dtype)),
        in_specs=[pl.BlockSpec(memory_space=pl.ANY)],
        out_specs=(vmem, vmem),
        scratch_shapes=[pltpu.SemaphoreType.DMA((2,))],
        name="fetch_halves",
    )(x)


def first_product(blocks, theirs, tile_rows, tile_cols):
    count, _, width = blocks.shape
    band, tile = count * tile_rows, theirs.shape[1]
    groups = tile_cols // 8

    def body(blocks_ref, theirs_ref, factor_ref, product_ref, turned_ref, sites_ref):
        r = lax.axis_index("row")
        for j in range(count):
            start = pl.multiple_of((r ^ j) * tile_rows, 8)
            factor_ref[pl.ds(start, tile_rows)] = blocks_ref[j, :tile_rows]
        product_ref[...] = product3(factor_ref[...], theirs_ref[...])
        for g in range(groups + 1):
            pieces = [blocks_ref[j, tile_rows:, g * tile_rows : (g + 1) * tile_rows] for j in range(count)]
            bit = 1
            while bit < count:
                pieces = [jnp.where((r & bit) != 0, pieces[j ^ bit], pieces[j]) for j in range(count)]
                bit *= 2
            row = jnp.concatenate(pieces, axis=1)
            if g < groups:
                turned_ref[8 * g : 8 * g + 8] = row
            else:
                sites_ref[...] = row

    vmem = pl.BlockSpec(memory_space=pltpu.VMEM)
    here = lambda *shape: pltpu.VMEM(shape, jnp.float32)
    return pl.pallas_call(
        body,
        out_shape=(here(band, width), here(band, tile), here(tile_cols, band), here(8, band)),
        in_specs=[vmem, vmem],
        out_specs=(vmem,) * 4,
        name="first_product",
    )(*[pltpu.with_memory_space_constraint(x, pltpu.VMEM) for x in (blocks, theirs)])


def left_product(rest, other, normal):
    band, tile = rest.shape

    def body(rest_ref, other_ref, normal_ref, out_ref):
        k = lax.axis_index("col") % 2
        right = split(normal_ref[...])
        for ref, half in ((rest_ref, k), (other_ref, 1 - k)):
            start = pl.multiple_of(half * tile, tile)
            out_ref[pl.ds(start, tile)] = dot3(split(ref[...].T), right)

    vmem = pl.BlockSpec(memory_space=pltpu.VMEM)
    return pl.pallas_call(
        body,
        out_shape=pltpu.VMEM((2 * tile, band), jnp.float32),
        in_specs=[vmem] * 3,
        out_specs=vmem,
        name="left_product",
    )(*[pltpu.with_memory_space_constraint(x, pltpu.VMEM) for x in (rest, other, normal)])


def finish(own, left, right, prior_covariance):
    tall, tile = prior_covariance.shape
    pieces = 2
    piece = tall // pieces

    def body(own_ref, left_ref, right_ref, prior_ref, rows_ref, out_ref, rows_buf, buf, sems):
        whole = split(right_ref[...])
        rows_buf[...] = dot3(split(own_ref[...]), whole)
        copies = [pltpu.make_async_copy(rows_buf, rows_ref, sems.at[pieces])]
        copies[0].start()
        for i in range(pieces):
            part = pl.ds(i * piece, piece)
            buf[part] = prior_ref[part] - dot3(split(left_ref[part]), whole)
            copies.append(pltpu.make_async_copy(buf.at[part], out_ref.at[part], sems.at[i]))
            copies[-1].start()
        for copy in copies:
            copy.wait()

    vmem = pl.BlockSpec(memory_space=pltpu.VMEM)
    hbm = pl.BlockSpec(memory_space=pl.ANY)
    rows_shape = (own.shape[0], tile)
    return pl.pallas_call(
        body,
        out_shape=(
            jax.ShapeDtypeStruct(rows_shape, jnp.float32),
            jax.ShapeDtypeStruct(prior_covariance.shape, jnp.float32),
        ),
        in_specs=[vmem] * 4,
        out_specs=(hbm, hbm),
        scratch_shapes=[
            pltpu.VMEM(rows_shape, jnp.float32),
            pltpu.VMEM(prior_covariance.shape, jnp.float32),
            pltpu.SemaphoreType.DMA((pieces + 1,)),
        ],
        name="finish",
    )(*[pltpu.with_memory_space_constraint(x, pltpu.VMEM) for x in (own, left, right, prior_covariance)])


def pack(prior_factor, band_factor, band_sites):
    height, width = prior_factor.shape
    turned = band_factor.T
    tall, wide = turned.shape
    groups = tall // 8

    def body(factor_ref, turned_ref, sites_ref, out_ref, turned_buf, sites_buf, sems):
        copies = [
            pltpu.make_async_copy(turned_ref, turned_buf, sems.at[0]),
            pltpu.make_async_copy(sites_ref, sites_buf, sems.at[1]),
            pltpu.make_async_copy(factor_ref, out_ref.at[pl.ds(0, height)], sems.at[2]),
        ]
        for copy in copies:
            copy.start()
        out_ref[height:, :] = jnp.zeros((8, width), jnp.float32)
        copies[0].wait()
        for i in range(groups):
            out_ref[height:, i * wide : (i + 1) * wide] = turned_buf[8 * i : 8 * i + 8, :]
        copies[1].wait()
        count, span = sites_buf.shape
        out_ref[height : height + count, groups * wide : groups * wide + span] = sites_buf[...]
        copies[2].wait()

    hbm = pl.BlockSpec(memory_space=pl.ANY)
    return pl.pallas_call(
        body,
        out_shape=pltpu.VMEM((height + 8, width), jnp.float32),
        in_specs=[hbm, hbm, hbm],
        out_specs=pl.BlockSpec(memory_space=pltpu.VMEM),
        scratch_shapes=[
            pltpu.VMEM(turned.shape, jnp.float32),
            pltpu.VMEM(band_sites.shape, jnp.float32),
            pltpu.SemaphoreType.DMA((3,)),
        ],
        name="pack",
    )(prior_factor, turned, band_sites)


def local(band_sites, test_sites, band_factor, prior_factor, prior_solution, prior_covariance):
    rows, cols = lax.axis_size("row"), lax.axis_size("col")
    tile = test_sites.shape[1]
    tile_rows, tile_cols = band_factor.shape
    band = tile_rows * rows
    r, c = lax.axis_index("row"), lax.axis_index("col")
    q, k = c // 2, c % 2

    def along_row(d):
        return lambda i, j: (i ^ d, j)

    def along_col(d):
        return lambda i, j: (i, j ^ (2 * d))

    def other_core(i, j):
        return i, j ^ 1

    def to_column(i, j):
        return matching(rows, i, j % 2 == 0)[j // 2], 2 * i + j % 2

    half, other_half = fetch_halves(prior_solution, tile)
    blocks = gather(pack(prior_factor, band_factor, band_sites), rows, cols, rows, along_row)
    factor, theirs, turned, sites = first_product(blocks, other_half, tile_rows, tile_cols)
    turned = turned.reshape(-1, tile)
    got = permute(jnp.concatenate([theirs, turned]), rows, cols, other_core)
    mine = dot(factor, half, precision=HIGH)
    cross = jnp.where(q == r, matern(sites, test_sites), 0.0)
    mine = lax.optimization_barrier(cross - mine)
    part = mine - got[:band]
    pair = natural(jnp.stack([turned, got[band:]]), k).reshape(-1, tile)

    rest, columns = reduce_and_gather(part, pair, rows, cols, cols // 2, along_col)
    moved = permute(rest, rows, cols, to_column)
    rest_other = permute(rest, rows, cols, other_core)
    triangle = natural(columns, q).reshape(band, band)
    if band <= 256:
        own, normal = invert(triangle, tile_rows)
    else:
        inverse = upper_inverse(triangle, dot)
        normal = dot(inverse, inverse, ((1,), (1,)))
        own = lax.dynamic_slice_in_dim(inverse, r * tile_rows, tile_rows, 1).T
    prior = fetch(prior_covariance)
    left = left_product(rest, rest_other, normal)
    return finish(own, left, jnp.where(q == r, rest, moved), prior)


def solution(mesh):
    placed = (
        P(None, "row"),
        P(None, "col"),
        P("row", "col"),
        P("row", "col"),
        P("col", "row"),
        P("row", "col"),
    )
    return jax.shard_map(
        local,
        mesh=mesh,
        in_specs=placed,
        out_specs=(P("row", "col"), P("row", "col")),
        check_vma=False,
    )
```
